32 devices in a mesh: rows: 32 (over z, y, x, core).
Axes of the slice: x: 2, y: 2, z: 4, core: 2. Of those that a mesh axis runs over, the one named last changes fastest.
Arguments:
- left_factor: float32 [65536, 1024], P('rows'), may hold values from -6 to 6
- right_factor: float32 [65536, 1024], P('rows'), may hold values from -6 to 6
- tile_counts: int32 [32], P('rows'), may hold values from 1 to 4, as said below
- start_basis: float32 [1024, 256], replicated, may hold values from -6 to 6
Outputs:
- left_proj: float32 [65536, 256], P('rows')
- right_proj: float32 [65536, 256], P('rows')
The draws below stay inside these ranges and needn't reach their ends.
Inputs may be any that keep to these rules, and one draw needn't show every extreme that they name: `tile_counts`: each device's live slots are its first ones; some device has 4 live slots and some device has 1.
All inputs are finite; a program needn't handle non-finite values.
Results may differ from the reference program's by a relative error of at most 0.0002.
Values sent between devices are 32-bit elements; how exact they have to be, the bound alone decides.
A program may use at most 128 MiB of HBM per device.

```python
import jax
import jax.numpy as jnp
from jax import lax

STATES = 1024
RANK = 256
TILE = 512
SLOTS = 4
POWER = 2
ROWS_ALL = 65536
N_ROWS = 32


def draw_tile_counts(key, part):
    kinds = jax.random.randint(jax.random.fold_in(key, 11), (N_ROWS,), 0, 4)
    middle = max(1, SLOTS // 2)
    counts = jnp.where(kinds < 2, 1, jnp.where(kinds == 2, middle, SLOTS)).astype(jnp.int32)
    heavy = jax.random.randint(jax.random.fold_in(key, 12), (), 0, N_ROWS)
    offset = jax.random.randint(jax.random.fold_in(key, 13), (), 1, N_ROWS)
    light = (heavy + offset) % N_ROWS
    positions = jnp.arange(N_ROWS, dtype=jnp.int32)
    counts = jnp.where(positions == heavy, SLOTS, counts)
    counts = jnp.where(positions == light, 1, counts)
    return counts.astype(jnp.int32)


def steps_of(rng, shape, pieces, least, high):
    loudness = 1.0
    for position, blocks in pieces:
        heights = jax.random.uniform(jax.random.fold_in(jax.random.fold_in(rng, 6), position), (blocks,), jnp.float32, least / len(pieces), high / len(pieces))
        loudness = loudness * jnp.repeat(jnp.exp(heights), shape[position] // blocks).reshape((-1,) + (1,) * (len(shape) - 1 - position))
    return loudness


def normal_values(key, extent, scale, reach, cuts=(), kind=jnp.bfloat16):
    result = scale * jax.random.normal(key, extent, jnp.float32)
    if cuts:
        result = result * steps_of(key, extent, cuts, -0.22, 0.18)
    return jnp.clip(result, -reach, reach).astype(kind)


def setup_inputs(seed: int = 0) -> dict:
    seeds = jax.random.split(jax.random.key(seed), 5)
    return {
        "left_factor": normal_values(seeds[0], (ROWS_ALL, STATES), 1.0, 6.0, ((0, 32),), jnp.float32),
        "right_factor": normal_values(seeds[1], (ROWS_ALL, STATES), 1.0, 6.0, ((0, 32),), jnp.float32),
        "tile_counts": draw_tile_counts(jax.random.fold_in(seeds[4], 71), 0),
        "start_basis": normal_values(seeds[3], (STATES, RANK), 1.0, 6.0, (), jnp.float32),
    }


def product(left_side, right_side):
    return jnp.dot(left_side.astype(jnp.float32), right_side.astype(jnp.float32), precision=lax.Precision.HIGHEST, preferred_element_type=jnp.float32)

def transposed_product(left_side, right_side):
    return lax.dot_general(left_side.astype(jnp.float32), right_side.astype(jnp.float32), (((0,), (0,)), ((), ())), precision=lax.Precision.HIGHEST, preferred_element_type=jnp.float32)

def right_solve(factor, block):
    return jax.scipy.linalg.solve_triangular(factor, block.T, lower=True).T

def orthonormal(block):
    factor = jnp.linalg.cholesky(transposed_product(block, block))
    return right_solve(factor, block)

def reference(left_factor, right_factor, tile_counts, start_basis):
    devices = tile_counts.shape[0]
    slot_ids = jnp.arange(SLOTS, dtype=jnp.int32)
    live_slots = (slot_ids[None, :] < tile_counts[:, None]).astype(left_factor.dtype)
    row_mask = jnp.broadcast_to(live_slots[:, :, None], (devices, SLOTS, TILE)).reshape(-1, 1)
    gram_matrix = transposed_product(left_factor, right_factor * row_mask)
    current = start_basis
    for iteration in range(POWER):
        current = orthonormal(transposed_product(gram_matrix, product(gram_matrix, current)))
    image_cols = product(gram_matrix, current)
    square = transposed_product(image_cols, image_cols)
    factor = jnp.linalg.cholesky(square)
    left_map = right_solve(factor, image_cols)
    scaling = jnp.sqrt(jnp.trace(square) / RANK)
    right_map = right_solve(factor, current) * scaling
    left_proj = product(left_factor, left_map) * row_mask
    right_proj = product(right_factor, right_map) * row_mask
    return (left_proj, right_proj)
```

```python
import functools

import jax
import jax.numpy as jnp
from jax import lax
from jax.experimental import pallas as pl
from jax.experimental.pallas import tpu as pltpu
from jax.sharding import PartitionSpec as P

SLOTS = 4
POWER = 2
GROUP = 8
MESH = pl.DeviceIdType.MESH
NN = (((1,), (0,)), ((), ()))
NT = (((1,), (1,)), ((), ()))


def split(value):
    high = value.astype(jnp.bfloat16)
    return high, (value - high.astype(jnp.float32)).astype(jnp.bfloat16)


def dot_pairs(left, right, dims):
    one = lambda a, b: lax.dot_general(a, b, dims, preferred_element_type=jnp.float32)
    return one(left[0], right[0]) + (one(left[0], right[1]) + one(left[1], right[0]))


def full_dot(left, right, dims=NN):
    return lax.dot_general(
        left, right, dims, precision=lax.Precision.HIGHEST, preferred_element_type=jnp.float32
    )


def sum_kernel(chips, part, high, low, arrived, summed, gathered, total, d2d, rs, ag, fwd):
    me = lax.axis_index("rows")
    core = lax.rem(me, 2)
    chip = me // 2
    partner = me + 1 - 2 * core
    half = part.shape[0] // 2
    rows = half // chips

    def block(which, owner):
        return pl.ds(pl.multiple_of(which * half + owner * rows, GROUP), rows)

    def ahead(u):
        return lax.rem(chip + u, chips)

    def behind(u):
        return lax.rem(chip + chips - u, chips)

    def copy(src, dst, sems, u, device):
        return pltpu.make_async_remote_copy(
            src_ref=src,
            dst_ref=dst,
            send_sem=sems.at[0, u - 1],
            recv_sem=sems.at[1, u - 1],
            device_id=(device,),
            device_id_type=MESH,
        )

    def to_partner(u):
        return copy(part.at[block(1 - core, ahead(u))], arrived.at[u - 1], d2d, u, partner)

    def to_owner(u):
        return copy(summed.at[u - 1], gathered.at[u - 1], rs, u, 2 * ahead(u) + core)

    def to_peer(u):
        mine = block(core, chip)
        return copy(total.at[mine], total.at[mine], ag, u, 2 * ahead(u) + core)

    def from_peer(u):
        theirs = block(core, behind(u))
        return copy(total.at[theirs], total.at[theirs], ag, u, 2 * behind(u) + core)

    def pass_on(u):
        theirs = block(core, behind(u))
        return copy(total.at[theirs], total.at[theirs], fwd, u, partner)

    def from_partner(u):
        theirs = block(1 - core, behind(u))
        return copy(total.at[theirs], total.at[theirs], fwd, u, partner)

    def each(first, last, body):
        def step(u, carry):
            body(u)
            return carry

        lax.fori_loop(first, last, step, 0)

    def put(where):
        pair = split(total[where])
        high[where] = pair[0]
        low[where] = pair[1]

    barrier = pltpu.get_barrier_semaphore()
    pl.semaphore_signal(barrier, inc=1, device_id=(partner,), device_id_type=MESH)
    each(
        1,
        chips,
        lambda u: pl.semaphore_signal(
            barrier, inc=1, device_id=(2 * ahead(u) + core,), device_id_type=MESH
        ),
    )
    pl.semaphore_wait(barrier, chips)

    each(1, chips + 1, lambda u: to_partner(u).start())

    def reduce_pair(u):
        to_partner(u).wait_recv()
        summed[u - 1] = part[block(core, ahead(u))] + arrived[u - 1]
        to_owner(u).start()

    each(1, chips, reduce_pair)
    to_partner(chips).wait_recv()
    mine = block(core, chip)
    total[mine] = part[mine] + arrived[chips - 1]

    def accumulate(u):
        to_owner(u).wait_recv()
        total[mine] += gathered[u - 1]

    each(1, chips, accumulate)
    each(1, chips, lambda u: to_peer(u).start())
    pass_on(chips).start()
    put(mine)

    def relay(u):
        from_peer(u).wait_recv()
        pass_on(u).start()
        put(block(core, behind(u)))

    each(1, chips, relay)
    from_partner(chips).wait_recv()
    put(block(1 - core, chip))

    def take(u):
        from_partner(u).wait_recv()
        put(block(1 - core, behind(u)))

    each(1, chips, take)
    each(1, chips + 1, lambda u: to_partner(u).wait_send())
    each(1, chips, lambda u: to_owner(u).wait_send())
    each(1, chips, lambda u: to_peer(u).wait_send())
    each(1, chips + 1, lambda u: pass_on(u).wait_send())


def sum_over_devices(part, devices):
    chips = devices // 2
    size, width = part.shape
    rows = size // devices
    block = pltpu.VMEM((chips, rows, width), jnp.float32)
    vmem = pl.BlockSpec(memory_space=pltpu.VMEM)
    sems = pltpu.SemaphoreType.DMA((2, chips))
    return pl.pallas_call(
        functools.partial(sum_kernel, chips),
        out_shape=[jax.ShapeDtypeStruct(part.shape, jnp.bfloat16)] * 2,
        in_specs=[vmem],
        out_specs=[vmem, vmem],
        scratch_shapes=[block, block, block, pltpu.VMEM(part.shape, jnp.float32), sems, sems, sems, sems],
        compiler_params=pltpu.CompilerParams(
            collective_id=0, has_side_effects=True, vmem_limit_bytes=40 * 2**20
        ),
        name="sum_over_devices",
    )(part)


def inverse_factor(matrix):
    size = matrix.shape[0]
    groups = size // GROUP
    shape = (GROUP, size)
    row_ids = lax.broadcasted_iota(jnp.int32, shape, 0)
    lane_ids = lax.broadcasted_iota(jnp.int32, shape, 1)
    wide = lambda v: jnp.broadcast_to(v, shape)
    left = [matrix[GROUP * g : GROUP * (g + 1), :] for g in range(groups)]
    right = [jnp.where(lane_ids == row_ids + GROUP * g, 1.0, 0.0) for g in range(groups)]
    for g in range(groups):
        panel, beside = left[g], right[g]
        entry, factor, inverse, scale = {}, {}, {}, {}
        for j in range(GROUP):
            column = wide(panel[:, GROUP * g + j : GROUP * g + j + 1])
            for i in range(j, GROUP):
                entry[i, j] = wide(column[i : i + 1, :])
        for j in range(GROUP):
            scale[j] = lax.rsqrt(entry[j, j])
            for i in range(j + 1, GROUP):
                factor[i, j] = entry[i, j] * scale[j]
            for l in range(j + 1, GROUP):
                for i in range(l, GROUP):
                    entry[i, l] = entry[i, l] - factor[i, j] * factor[l, j]
        for j in range(GROUP):
            inverse[j, j] = scale[j]
            for i in range(j + 1, GROUP):
                acc = factor[i, j] * inverse[j, j]
                for l in range(j + 1, i):
                    acc = acc + factor[i, l] * inverse[l, j]
                inverse[i, j] = -acc * scale[i]
        new_panel, new_beside = jnp.zeros(shape, jnp.float32), jnp.zeros(shape, jnp.float32)
        for j in range(GROUP):
            column = jnp.zeros(shape, jnp.float32)
            for i in range(j, GROUP):
                column = jnp.where(row_ids == i, inverse[i, j], column)
            new_panel = new_panel + column * wide(panel[j : j + 1, :])
            new_beside = new_beside + column * wide(beside[j : j + 1, :])
        right[g] = new_beside
        if g + 1 < groups:
            turned = new_panel.T
            rows_of = [wide(new_panel[j : j + 1, :]) for j in range(GROUP)]
            beside_of = [wide(new_beside[j : j + 1, :]) for j in range(GROUP)]
            for r in range(g + 1, groups):
                tile = turned[GROUP * r : GROUP * (r + 1), :]
                for j in range(GROUP):
                    weight = wide(tile[:, j : j + 1])
                    left[r] = left[r] - weight * rows_of[j]
                    right[r] = right[r] - weight * beside_of[j]
    return jnp.concatenate(right, axis=0)


def chain_kernel(start, high, low, left_map, right_map, basis, image, square, inverse):
    rank = start.shape[0]
    cut = rank // 2
    basis[...] = start[...]
    inverse[...] = jnp.zeros_like(inverse)

    def turn(iteration, carry):
        gram = (high[...], low[...])
        image[...] = dot_pairs(split(basis[...]), gram, NT)

        @pl.when(iteration < POWER)
        def _():
            image[...] = dot_pairs(split(image[...]), (high[...], low[...]), NN)

        pair = split(image[...])
        square[...] = dot_pairs(pair, pair, NT)
        first = inverse_factor(square[:cut, :cut])
        across = full_dot(first, square[:cut, cut:])
        across_t = across.T
        second = inverse_factor(square[cut:, cut:] - full_dot(across_t, across))
        inverse[:cut, :cut] = first
        inverse[cut:, cut:] = second
        inverse[cut:, :cut] = -full_dot(second, full_dot(across_t, first))
        solved = split(inverse[...])

        @pl.when(iteration == POWER)
        def _():
            shape = square.shape
            diagonal = lax.broadcasted_iota(jnp.int32, shape, 0) == lax.broadcasted_iota(jnp.int32, shape, 1)
            trace = jnp.sum(jnp.where(diagonal, square[...], 0.0), keepdims=True)
            scaling = jnp.sqrt(trace / rank)
            right_map[...] = dot_pairs(solved, split(basis[...]), NN) * scaling
            left_map[...] = dot_pairs(solved, pair, NN)

        @pl.when(iteration < POWER)
        def _():
            basis[...] = dot_pairs(solved, pair, NN)

        return carry

    lax.fori_loop(0, POWER + 1, turn, 0)


def maps_of(start_rows, high, low):
    rank, states = start_rows.shape
    vmem = pl.BlockSpec(memory_space=pltpu.VMEM)
    small = pltpu.VMEM((rank, rank), jnp.float32)
    wide = pltpu.VMEM((rank, states), jnp.float32)
    return pl.pallas_call(
        chain_kernel,
        out_shape=[jax.ShapeDtypeStruct((rank, states), jnp.float32)] * 2,
        in_specs=[vmem] * 3,
        out_specs=[vmem] * 2,
        scratch_shapes=[wide, wide, small, small],
        compiler_params=pltpu.CompilerParams(vmem_limit_bytes=40 * 2**20),
        name="maps_of",
    )(start_rows, high, low)


def project(factor_rows, mapping, row_mask):
    rows = lax.dot_general(
        factor_rows, mapping, NT, precision=lax.Precision.HIGH, preferred_element_type=jnp.float32
    )
    return rows * row_mask


def local(devices, left_factor, right_factor, tile_counts, start_basis):
    tile_rows = left_factor.shape[0] // SLOTS
    live_count = tile_counts[0]
    slot_ids = lax.broadcasted_iota(jnp.int32, (SLOTS, 1, 1), 0)
    live_slots = (slot_ids < live_count).astype(jnp.float32)
    row_mask = jnp.broadcast_to(live_slots, (SLOTS, tile_rows, 1)).reshape(-1, 1)
    part = lax.dot_general(
        left_factor,
        right_factor * row_mask,
        (((0,), (0,)), ((), ())),
        precision=lax.Precision.HIGH,
        preferred_element_type=jnp.float32,
    )
    high, low = sum_over_devices(part, devices)
    left_map, right_map = maps_of(start_basis.T, high, low)
    return project(left_factor, left_map, row_mask), project(right_factor, right_map, row_mask)


def solution(mesh):
    return jax.shard_map(
        functools.partial(local, mesh.shape["rows"]),
        mesh=mesh,
        in_specs=(P("rows", None), P("rows", None), P("rows"), P()),
        out_specs=(P("rows", None), P("rows", None)),
        check_vma=False,
    )
```
